256 devices in a mesh: subj: 4 (over x, y), gx: 32 (over z), gy: 2 (over core).
Axes of the slice: x: 2, y: 2, z: 32, core: 2. Of those that a mesh axis runs over, the one named last changes fastest.
The devices are a block of a 4x8x32 slice.
Arguments:
- bold: float32 [1200, 128, 64, 32], P('subj', 'gx', 'gy'), parts along dimension 0, may hold values from -70 to 70
- brain_bounds: int32 [128, 64, 8], P('gx', 'gy', 'subj'), parts along dimension 2, may hold values from 0 to 32, as said below
- seed_index: int32 [4096], P('subj'), parts along dimension 0, may hold values from 0 to 262143
Outputs:
- connectivity: bfloat16 [128, 64, 32, 4096], P('gx', 'gy', None, 'subj'), parts along dimension 3
The draws below stay inside these ranges and needn't reach their ends.
There are 4 independent parts, one for each index of `subj`. The reference program is written for one: setup_inputs(seed, part) draws one part's arguments, and reference() takes and returns one part's arrays. A program takes and returns all parts, laid end to end along the dimension named above; each array names one. Nothing has to cross between parts.
Inputs may be any that keep to these rules, and one draw needn't show every extreme that they name: `brain_bounds`: in every column the first bound is at most 16 and the second at least 16. `seed_index`: voxel number (x * 64 + y) * 32 + z; seeds may repeat.
All inputs are finite; a program needn't handle non-finite values.
Results may differ from the reference program's by a relative error of at most 0.0056.
Values may be sent and summed in bfloat16 or wider, within the bound.
No kernel may reach another device: no remote copies, remote signals or barrier semaphores. Data moves between devices by JAX's collectives and lax.ppermute only.
A program may use at most 128 MiB of HBM per device.

```python
import math
import jax
import jax.numpy as jnp
from jax import lax

FRAMES = 300
SEEDS = 1024
NZ = 32
NX = 128
NY = 64
VOXELS = 262144


def draw_bold(key, part):
    first, second, third = jax.random.split(key, 3)
    shape = (FRAMES, NX, NY, NZ)
    scale = jnp.exp(jax.random.uniform(first, (1, NX, NY, NZ), minval=0.0, maxval=math.log(10.0)))
    base = jnp.clip(3.0 * jax.random.normal(second, (1, NX, NY, NZ)), -12.0, 12.0)
    noise = jnp.clip(jax.random.normal(third, shape), -5.0, 5.0)
    return (base + scale * noise).astype(jnp.float32)


def draw_brain_bounds(key, part):
    first, second = jax.random.split(jax.random.fold_in(key, 17))
    across = (2 * jnp.arange(NX, dtype=jnp.int32) - NX + 1) * 64 // NX
    down = (2 * jnp.arange(NY, dtype=jnp.int32) - NY + 1) * 64 // NY
    radius = across[:, None] * across[:, None] + down[None, :] * down[None, :]
    half = jnp.maximum(NZ // 2 * (4096 - radius) // 4096, 0)
    below = jax.random.randint(first, (NX, NY), 0, NZ // 8 + 1)
    above = jax.random.randint(second, (NX, NY), 0, NZ // 8 + 1)
    lower = jnp.clip(NZ // 2 - half - below, 0, NZ // 2)
    upper = jnp.clip(NZ // 2 + half + above, NZ // 2, NZ)
    return jnp.stack([lower, upper], axis=-1).astype(jnp.int32)


def place_ends(entries, own_key, low, top_value):
    longest = entries.shape.index(max(entries.shape))
    spots = []
    for shift in (0, 1):
        where = [jax.random.randint(jax.random.fold_in(own_key, axis), (), 0, length) for axis, length in enumerate(entries.shape)]
        where[longest] = (where[longest] + shift) % entries.shape[longest]
        spots.append(tuple(where))
    return entries.at[spots[0]].set(low).at[spots[1]].set(top_value)


def setup_inputs(seed: int = 0, part: int = 0) -> dict:
    keys = jax.random.split(jax.random.key(seed), 4)
    part_splits = jax.random.split(jax.random.fold_in(keys[3], part), 4)
    bold = draw_bold(jax.random.fold_in(jax.random.fold_in(keys[3], part), 71), part)
    brain_bounds = draw_brain_bounds(jax.random.fold_in(jax.random.fold_in(keys[3], part), 71), part)
    seed_index = place_ends(jax.random.randint(part_splits[2], (SEEDS,), 0, VOXELS), jax.random.fold_in(part_splits[2], 1), 0, VOXELS - 1).astype(jnp.int32)
    return dict(bold=bold, brain_bounds=brain_bounds, seed_index=seed_index)


raw_taps = [math.exp(-k * k / 8.0) for k in range(-4, 5)]
kernel_taps = [t / sum(raw_taps) for t in raw_taps]

def smooth_axis(padded, axis, count):
    total = kernel_taps[0] * lax.slice_in_dim(padded, 0, count, axis=axis)
    for k in range(1, 9):
        total = total + kernel_taps[k] * lax.slice_in_dim(padded, k, k + count, axis=axis)
    return total

def pad_axis(field, axis):
    widths = [(0, 0)] * field.ndim
    widths[axis] = (4, 4)
    return jnp.pad(field, widths)

def reference(bold, brain_bounds, seed_index):
    frames, nx_cells, ny_cells, nz_cells = bold.shape
    along_x = smooth_axis(pad_axis(bold, 1), 1, nx_cells)
    along_y = smooth_axis(pad_axis(along_x, 2), 2, ny_cells)
    smoothed = smooth_axis(pad_axis(along_y, 3), 3, nz_cells)
    mean = lax.optimization_barrier(jnp.mean(smoothed, axis=0))
    centered = smoothed - mean
    var = lax.optimization_barrier(jnp.mean(centered * centered, axis=0))
    zscored = (centered * lax.rsqrt(var + 1e-06)).astype(jnp.bfloat16)
    flat = zscored.reshape(frames, nx_cells * ny_cells * nz_cells)
    table = jnp.take(flat, seed_index.astype(jnp.int32), axis=1)
    planes = jnp.moveaxis(zscored, 1, 0).reshape(nx_cells, frames, ny_cells * nz_cells)
    depth = jnp.arange(nz_cells, dtype=jnp.int32)
    inside = (depth[None, None, :] >= brain_bounds[:, :, 0:1]) & (depth[None, None, :] < brain_bounds[:, :, 1:2])

    def one_plane(packed):
        plane, keep = packed
        corr = lax.dot_general(plane, table, (((0,), (0,)), ((), ())), preferred_element_type=jnp.float32)
        corr = corr * (1.0 / frames)
        corr = corr.reshape(ny_cells, nz_cells, -1) * keep[:, :, None].astype(jnp.float32)
        return corr.astype(jnp.bfloat16)
    return lax.map(one_plane, (planes, inside))
```

```python
import functools
import math

import jax
import jax.numpy as jnp
import numpy as np
from jax import lax
from jax.experimental import pallas as pl
from jax.experimental.pallas import tpu as pltpu
from jax.sharding import PartitionSpec as P


raw_taps = [math.exp(-k * k / 8.0) for k in range(-4, 5)]
kernel_taps = [t / sum(raw_taps) for t in raw_taps]
TAP_SUM = sum(raw_taps)
REACH = 4
LANES = 128
BF = jnp.bfloat16
F32 = jnp.float32
PAIRS = (4, 8, 4)
NCHUNK = len(PAIRS)
HALF = 32
LIST = 2 * HALF
VMEM = 56 * 1024 * 1024


def dot(a, b, dims=(((1,), (0,)), ((), ()))):
    return lax.dot_general(a, b, dims, preferred_element_type=F32)


def split(a):
    high = a.astype(BF)
    return high, (a - high.astype(F32)).astype(BF)


def in_plane_kernel(side_ref, bold_ref, edge_ref, high_ref, low_ref, *refs, frames):
    chunks, rests, wide = refs[:NCHUNK], refs[NCHUNK : 2 * NCHUNK], refs[2 * NCHUNK]
    rows, cells_z = bold_ref.shape[1], bold_ref.shape[2]
    lanes = wide.shape[2]
    keep = lax.broadcasted_iota(jnp.int32, (1, 1, lanes), 2) < frames
    side = side_ref[0]
    taps_high, taps_low = high_ref[...], low_ref[...]
    group = taps_high.shape[0] // cells_z

    def along_z(block, count):
        block = jnp.where(keep, block, 0.0)
        mean = jnp.sum(block, axis=-1, keepdims=True) * (1.0 / frames)
        block = jnp.where(keep, block - mean, 0.0).reshape(count * cells_z, lanes)
        size = count * cells_z
        head, rest = split(block)
        th, tl = taps_high[:size, :size], taps_low[:size, :size]
        return (dot(th, head) + dot(th, rest) + dot(tl, head)).reshape(count, cells_z, lanes)

    for at in range(0, rows, group):
        wide[REACH + at : REACH + at + group] = along_z(bold_ref[0, at : at + group], group)
    edge = along_z(edge_ref[0], REACH)
    wide[:REACH] = jnp.where(side == 1, edge, 0.0)
    wide[REACH + rows :] = jnp.where(side == 1, 0.0, edge)

    def one_pair(index, at):
        first_row = 2 * (sum(PAIRS[:index]) + at)

        def along_y(row):
            total = kernel_taps[REACH] * wide[row + REACH]
            for k in range(1, REACH + 1):
                total = total + kernel_taps[REACH + k] * (wide[row + REACH - k] + wide[row + REACH + k])
            return total

        first, second = along_y(first_row), along_y(first_row + 1)
        last = first[:, 2 * LANES :] + pltpu.roll(second[:, 2 * LANES :], LANES // 2, 1)
        pieces = (first[:, :LANES], first[:, LANES : 2 * LANES], second[:, :LANES], second[:, LANES : 2 * LANES], last)
        for k, piece in enumerate(pieces):
            head, tail = split(piece)
            chunks[index][k, 0, at] = head
            rests[index][k, 0, at] = tail

    for index in range(NCHUNK):
        lax.fori_loop(0, PAIRS[index], lambda at, _, index=index: one_pair(index, at), None)


def in_plane(bold, edge, side):
    cells_x, cells_y, cells_z, frames = bold.shape
    group = 256 // cells_z
    band = np.zeros((cells_z, cells_z), np.float64)
    for k in range(-REACH, REACH + 1):
        band += kernel_taps[k + REACH] * np.eye(cells_z, k=k)
    band = np.kron(np.eye(group), band).astype(np.float32)
    high = band.astype(BF)
    low = (band - high.astype(np.float32)).astype(BF)
    lanes = 3 * LANES
    pieces = [jax.ShapeDtypeStruct((5, cells_x, pairs, cells_z, LANES), BF) for pairs in PAIRS]
    piece_specs = [pl.BlockSpec((5, 1) + piece.shape[2:], lambda x: (0, x, 0, 0, 0)) for piece in pieces]
    whole = pl.BlockSpec(high.shape, lambda x: (0, 0))
    outs = pl.pallas_call(
        functools.partial(in_plane_kernel, frames=frames),
        grid=(cells_x,),
        in_specs=[
            pl.BlockSpec(memory_space=pltpu.SMEM),
            pl.BlockSpec((1, cells_y, cells_z, lanes), lambda x: (x, 0, 0, 0)),
            pl.BlockSpec((1, REACH, cells_z, lanes), lambda x: (x, 0, 0, 0)),
            whole,
            whole,
        ],
        out_specs=piece_specs * 2,
        out_shape=pieces * 2,
        scratch_shapes=[pltpu.VMEM((cells_y + 2 * REACH, cells_z, lanes), F32)],
        compiler_params=pltpu.CompilerParams(vmem_limit_bytes=VMEM),
        name="in_plane",
    )(side, bold, edge, jnp.asarray(high), jnp.asarray(low))
    return outs[:NCHUNK], outs[NCHUNK:]


def rank_kernel(row_ref, out_ref, turns_ref, *, column):
    seeds, chips = row_ref.shape[1], out_ref.shape[0]
    seed = row_ref[...]
    chip = lax.broadcasted_iota(jnp.int32, (chips, 1), 0) * column
    here = jnp.where((seed >= chip) & (seed < chip + column), 1.0, 0.0)
    earlier = lax.broadcasted_iota(jnp.int32, (seeds, seeds), 0) < lax.broadcasted_iota(jnp.int32, (seeds, seeds), 1)
    before = dot(here.astype(BF), jnp.where(earlier, 1.0, 0.0).astype(BF))
    rank = jnp.sum(here * before, axis=0, keepdims=True)
    out_ref[...] = jnp.broadcast_to(rank.astype(jnp.int32), out_ref.shape)
    turns_ref[0] = (jnp.max(rank).astype(jnp.int32) + LIST) // LIST


def part_kernel(place_ref, row_ref, rank_ref, *refs, cells, column, strip):
    chunks, rests, outs = refs[:NCHUNK], refs[NCHUNK : 2 * NCHUNK], refs[2 * NCHUNK :]
    cells_x, cells_y, cells_z = cells
    brick, side, turn = place_ref[0], place_ref[1], place_ref[2]
    half = 3 * HALF
    slots = 2 * half
    seed = row_ref[...]
    rank = rank_ref[0:1] - turn * LIST
    spot = jnp.where((rank >= 0) & (rank < LIST), (seed // column) * LIST + rank, -1)
    slot = lax.broadcasted_iota(jnp.int32, (slots, 1), 0)
    core = jnp.where(slot < half, side, 1 - side)
    slot = jnp.where(slot < half, slot, slot - half)
    which = jnp.where(slot < HALF, 0, jnp.where(slot < 2 * HALF, 1, 2))
    want = (brick - 1 + which) * LIST + core * HALF + slot - which * HALF
    want = jnp.where(want >= 0, want, -2)
    found = jnp.sum(jnp.where(spot == want, (seed + 1).astype(F32), 0.0), axis=1, keepdims=True)
    found = found.astype(jnp.int32) - 1
    seed_x = found // strip
    within = found - seed_x * strip
    seed_y = within // cells_z
    seed_z = within - seed_y * cells_z
    from_x = seed_x - brick * cells_x
    from_y = jnp.where(found < 0, -1, seed_y - side * cells_y)

    main = jnp.zeros((slots, 2 * LANES), F32)
    last = jnp.zeros((2 * slots, LANES), F32)

    def product(weights, index, pieces):
        head, tail = (
            jnp.concatenate([refs[index][k].reshape(-1, LANES) for k in pieces], axis=1) for refs in (chunks, rests)
        )
        high, low = weights
        return dot(high, head) + dot(high, tail) + dot(low, head)

    for index, pairs in enumerate(PAIRS):
        lane = lax.broadcasted_iota(jnp.int32, (1, cells_x * pairs * cells_z), 1)
        shift_z, shift_p = cells_z.bit_length() - 1, pairs.bit_length() - 1
        row = 2 * (((lane >> shift_z) & (pairs - 1)) + sum(PAIRS[:index]))
        gap = ((lane >> (shift_z + shift_p)) - from_x).astype(F32)
        taps = jnp.where(jnp.abs(gap) <= REACH, jnp.exp(gap * gap * (-1.0 / 8.0)) * (1.0 / TAP_SUM), 0.0)
        taps = jnp.where((lane & (cells_z - 1)) == seed_z, taps, 0.0)
        both = [split(jnp.where(row + odd == from_y, taps, 0.0)) for odd in range(2)]
        main = main + product(both[0], index, (0, 1)) + product(both[1], index, (2, 3))
        last = last + product([jnp.concatenate(w, axis=0) for w in zip(*both)], index, (4,))
    near = lax.broadcasted_iota(jnp.int32, (1, LANES), 1) < LANES // 2
    last = jnp.where(near, last[:slots] + pltpu.roll(last[slots:], LANES // 2, 1), 0.0)
    for k, out_ref in enumerate(outs):
        out_ref[:, : 2 * LANES] = main[k * half : (k + 1) * half]
        out_ref[:, 2 * LANES :] = last[k * half : (k + 1) * half]


def sum_kernel(own_ref, other_ref, *outs):
    for k, out_ref in enumerate(outs):
        rows = slice(k * HALF, (k + 1) * HALF)
        out_ref[...] = own_ref[rows] + other_ref[rows]


def scale_kernel(*refs, frames):
    ins, out_ref = refs[:-1], refs[-1]
    total = ins[0][...]
    for ref in ins[1:]:
        total = total + ref[...]
    var = jnp.sum(total * total, axis=1, keepdims=True) * (1.0 / frames)
    total = total * lax.rsqrt(var + 1e-06)
    half = HALF // 2
    first, second = total[:half], total[half:]
    last = first[:, 2 * LANES :] + pltpu.roll(second[:, 2 * LANES :], LANES // 2, 1)
    pieces = (first[:, :LANES], first[:, LANES : 2 * LANES], second[:, :LANES], second[:, LANES : 2 * LANES], last)
    for k, piece in enumerate(pieces):
        out_ref[0, k] = piece.astype(BF)


def order_kernel(place_ref, row_ref, rank_ref, own_ref, other_ref, out_ref, *, column):
    side, turn = place_ref[1], place_ref[2]
    half = HALF // 2
    count = own_ref.shape[0] * half
    rank = rank_ref[0:1] - turn * LIST
    quarter = sum(jnp.where(rank >= k * half, 1, 0) for k in range(1, 4))
    part = jnp.where(side == 0, quarter, jnp.where(quarter < 2, quarter + 2, quarter - 2))
    spot = part * count + (row_ref[...] // column) * half + rank - quarter * half
    spot = jnp.where((rank >= 0) & (rank < LIST), spot, -1)
    slot = lax.broadcasted_iota(jnp.int32, (count, 1), 0)
    picks = [jnp.where(spot - part * count == slot, 1.0, 0.0).astype(BF) for part in range(4)]

    def piece(part, k):
        ref = (own_ref, other_ref)[part // 2]
        return dot(ref[:, k].reshape(count, LANES), picks[part], (((0,), (0,)), ((), ())))

    for k in range(2):
        value = piece(0, k) + piece(1, 2 + k) + piece(2, k) + piece(3, 2 + k)
        out_ref[k * LANES : (k + 1) * LANES] = value.astype(BF)
    even, odd = piece(0, 4) + piece(2, 4), piece(1, 4) + piece(3, 4)
    last = even[: LANES // 2] + odd[LANES // 2 :]
    out_ref[2 * LANES :] = jnp.concatenate([last, jnp.zeros_like(last)], axis=0).astype(BF)


def in_order(place, row, ranks, own, other, column):
    seeds, block = row.shape[1], 256
    return pl.pallas_call(
        functools.partial(order_kernel, column=column),
        grid=(seeds // block,),
        in_specs=[
            pl.BlockSpec(memory_space=pltpu.SMEM),
            pl.BlockSpec((1, block), lambda i: (0, i)),
            pl.BlockSpec((ranks.shape[0], block), lambda i: (0, i)),
        ]
        + [pl.BlockSpec(own.shape, lambda i: (0, 0, 0, 0))] * 2,
        out_specs=pl.BlockSpec((3 * LANES, block), lambda i: (0, i)),
        out_shape=jax.ShapeDtypeStruct((3 * LANES, seeds), BF),
        compiler_params=pltpu.CompilerParams(vmem_limit_bytes=VMEM),
        name="order",
    )(place, row, ranks, own, other)


def finish_kernel(bounds_ref, table_ref, own_ref, before_ref, after_ref, *refs, frames, first):
    out_ref = refs[-1]
    cells_x, cells_z = own_ref.shape[1], own_ref.shape[3]
    pair = first + pl.program_id(0)
    near = lax.broadcasted_iota(jnp.int32, (1, LANES), 1) < LANES // 2
    depth = lax.broadcasted_iota(jnp.int32, (cells_z, 1), 0)
    table = table_ref[...]

    def plane(k, x):
        if x < 0:
            return before_ref[k, x + cells_x, 0].astype(F32)
        if x >= cells_x:
            return after_ref[k, x - cells_x, 0].astype(F32)
        return own_ref[k, x, 0].astype(F32)

    rows = []
    for x in range(cells_x):
        sums = []
        for k in range(5):
            total = kernel_taps[REACH] * plane(k, x)
            for t in range(1, REACH + 1):
                total = total + kernel_taps[REACH + t] * (plane(k, x - t) + plane(k, x + t))
            sums.append(total)
        for odd in range(2):
            last = pltpu.roll(sums[4], LANES // 2, 1) if odd else sums[4]
            pieces = (sums[2 * odd], sums[2 * odd + 1], jnp.where(near, last, 0.0))
            square = pieces[0] * pieces[0] + pieces[1] * pieces[1] + pieces[2] * pieces[2]
            var = jnp.sum(square, axis=1, keepdims=True) * (1.0 / frames)
            row = x * (bounds_ref.shape[1] // cells_x) + 2 * pair + odd
            inside = (depth >= bounds_ref[0, row]) & (depth < bounds_ref[1, row])
            scale = jnp.where(inside, lax.rsqrt(var + 1e-06), 0.0)
            rows.append(jnp.concatenate([(p * scale).astype(BF) for p in pieces], axis=1))
    corr = dot(jnp.concatenate(rows, axis=0), table) * (1.0 / frames)
    out_ref[...] = corr.astype(BF).reshape(out_ref.shape)


def finish(bounds, table, own, before, after, out, shape, frames, chunk):
    _, cells_x, pairs, cells_z, _ = own.shape
    first = sum(PAIRS[:chunk])
    spec = pl.BlockSpec((5, cells_x, 1, cells_z, LANES), lambda p: (0, 0, p, 0, 0))
    more = [] if out is None else [out]
    return pl.pallas_call(
        functools.partial(finish_kernel, frames=frames, first=first),
        grid=(pairs,),
        in_specs=[
            pl.BlockSpec(memory_space=pltpu.SMEM),
            pl.BlockSpec(table.shape, lambda p: (0, 0)),
            spec,
            spec,
            spec,
        ]
        + [pl.BlockSpec(memory_space=pl.ANY)] * len(more),
        out_specs=pl.BlockSpec((cells_x, 2, cells_z, shape[-1]), lambda p: (0, first + p, 0, 0)),
        out_shape=jax.ShapeDtypeStruct(shape, BF),
        input_output_aliases={5: 0} if more else {},
        compiler_params=pltpu.CompilerParams(vmem_limit_bytes=VMEM),
        name="finish",
    )(bounds, table, own, before, after, *more)


def call(kernel, out, *args, smem=0):
    in_specs = [pl.BlockSpec(memory_space=pltpu.SMEM)] * smem + [pl.BlockSpec(memory_space=pltpu.VMEM)] * (len(args) - smem)
    multi = isinstance(out, list)
    return pl.pallas_call(
        kernel,
        in_specs=in_specs,
        out_specs=[pl.BlockSpec(memory_space=pltpu.VMEM)] * len(out) if multi else pl.BlockSpec(memory_space=pltpu.VMEM),
        out_shape=out,
        compiler_params=pltpu.CompilerParams(vmem_limit_bytes=VMEM),
    )(*args)


def shift(value, step, flip=False, wrap=False):
    size, cores = lax.axis_size("gx"), lax.axis_size("gy")
    pairs = []
    for i in range(size):
        if wrap or 0 <= i + step < size:
            for c in range(cores):
                source = (i + step) % size * cores + (cores - 1 - c if flip else c)
                pairs.append((source, i * cores + c))
    return lax.ppermute(value, ("gx", "gy"), pairs)


def local(bold, brain_bounds, seed_index):
    frames, cells_x, cells_y, cells_z = bold.shape
    seeds = seed_index.shape[0]
    size, cores = lax.axis_size("gx"), lax.axis_size("gy")
    brick, side = lax.axis_index("gx"), lax.axis_index("gy")
    bold = jnp.transpose(bold, (1, 2, 3, 0))
    sides = side.astype(jnp.int32).reshape(1)

    send = lax.dynamic_slice_in_dim(bold, jnp.where(side == 0, cells_y - REACH, 0), REACH, axis=1)
    edge = shift(send, 0, flip=True)
    bounds = jnp.transpose(brain_bounds, (2, 0, 1)).reshape(2, cells_x * cells_y)
    edge, bounds = lax.optimization_barrier((edge, bounds))
    chunks, rests = in_plane(bold, edge, sides)
    halos = [(shift(c, -1), shift(c, 1)) for c in chunks]

    strip = cores * cells_y * cells_z
    column = cells_x * strip
    row = seed_index.reshape(1, seeds)
    ranks, turns = pl.pallas_call(
        functools.partial(rank_kernel, column=column),
        in_specs=[pl.BlockSpec(memory_space=pltpu.VMEM)],
        out_specs=[pl.BlockSpec(memory_space=pltpu.VMEM), pl.BlockSpec(memory_space=pltpu.SMEM)],
        out_shape=[jax.ShapeDtypeStruct((size, seeds), jnp.int32), jax.ShapeDtypeStruct((1,), jnp.int32)],
        name="rank",
    )(row)

    def table_of(turn):
        place = jnp.stack([brick, side, turn]).astype(jnp.int32)
        own, other = call(
            functools.partial(part_kernel, cells=(cells_x, cells_y, cells_z), column=column, strip=strip),
            [jax.ShapeDtypeStruct((3 * HALF, 3 * LANES), F32)] * 2,
            place,
            row,
            ranks,
            *chunks,
            *rests,
            smem=1,
        )
        other = shift(other, 0, flip=True)
        lists = call(sum_kernel, [jax.ShapeDtypeStruct((HALF, 3 * LANES), F32)] * 3, own, other)
        below = shift(lists[2], -1)
        above = shift(lists[0], 1)
        mine = call(
            functools.partial(scale_kernel, frames=frames),
            jax.ShapeDtypeStruct((1, 5, HALF // 2, LANES), BF),
            lists[1],
            below,
            above,
        )
        every = lax.all_gather(mine, "gx", axis=0, tiled=True)
        other = shift(every, 0, flip=True)
        return in_order(place, row, ranks, every, other, column)

    table = table_of(jnp.int32(0))
    _, table = lax.while_loop(
        lambda s: s[0] < turns[0], lambda s: (s[0] + 1, s[1] + table_of(s[0])), (jnp.int32(1), table)
    )

    shape = (cells_x, cells_y, cells_z, seeds)
    out = None
    for index in range(NCHUNK):
        out = finish(bounds, table, chunks[index], *halos[index], out, shape, frames, index)
    return out


def solution(mesh):
    placed = (P("subj", "gx", "gy", None), P("gx", "gy", "subj"), P("subj"))

    return jax.shard_map(local, mesh=mesh, in_specs=placed, out_specs=P("gx", "gy", None, "subj"), check_vma=False)
```

```python
import functools
import math

import jax
import jax.numpy as jnp
import numpy as np
from jax import lax
from jax.experimental import pallas as pl
from jax.experimental.pallas import tpu as pltpu
from jax.sharding import PartitionSpec as P


raw_taps = [math.exp(-k * k / 8.0) for k in range(-4, 5)]
kernel_taps = [t / sum(raw_taps) for t in raw_taps]
TAP_SUM = sum(raw_taps)
REACH = 4
LANES = 128
BF = jnp.bfloat16
F32 = jnp.float32
PAIRS = (4, 4, 4, 4)
NCHUNK = len(PAIRS)
HALF = 32
LIST = 2 * HALF
VMEM = 56 * 1024 * 1024


def dot(a, b, dims=(((1,), (0,)), ((), ()))):
    return lax.dot_general(a, b, dims, preferred_element_type=F32)


def split(a):
    high = a.astype(BF)
    return high, (a - high.astype(F32)).astype(BF)


def in_plane_kernel(side_ref, bold_ref, edge_ref, high_ref, low_ref, *refs, frames):
    chunks, rests, wide = refs[:NCHUNK], refs[NCHUNK : 2 * NCHUNK], refs[2 * NCHUNK]
    rows, cells_z = bold_ref.shape[1], bold_ref.shape[2]
    lanes = wide.shape[2]
    keep = lax.broadcasted_iota(jnp.int32, (1, 1, lanes), 2) < frames
    side = side_ref[0]
    taps_high, taps_low = high_ref[...], low_ref[...]
    group = taps_high.shape[0] // cells_z

    def along_z(block, count):
        block = jnp.where(keep, block, 0.0)
        mean = jnp.sum(block, axis=-1, keepdims=True) * (1.0 / frames)
        block = jnp.where(keep, block - mean, 0.0).reshape(count * cells_z, lanes)
        size = count * cells_z
        head, rest = split(block)
        th, tl = taps_high[:size, :size], taps_low[:size, :size]
        return (dot(th, head) + dot(th, rest) + dot(tl, head)).reshape(count, cells_z, lanes)

    def two_groups(step, _):
        for k in range(2):
            at = (2 * step + k) * group
            wide[pl.ds(REACH + at, group)] = along_z(bold_ref[0, pl.ds(at, group)], group)

    lax.fori_loop(0, rows // group // 2, two_groups, None)
    edge = along_z(edge_ref[0], REACH)
    wide[:REACH] = jnp.where(side == 1, edge, 0.0)
    wide[REACH + rows :] = jnp.where(side == 1, 0.0, edge)

    def one_pair(index, at):
        first_row = 2 * (sum(PAIRS[:index]) + at)

        def along_y(row):
            total = kernel_taps[REACH] * wide[row + REACH]
            for k in range(1, REACH + 1):
                total = total + kernel_taps[REACH + k] * (wide[row + REACH - k] + wide[row + REACH + k])
            return total

        first, second = along_y(first_row), along_y(first_row + 1)
        last = first[:, 2 * LANES :] + pltpu.roll(second[:, 2 * LANES :], LANES // 2, 1)
        pieces = (first[:, :LANES], first[:, LANES : 2 * LANES], second[:, :LANES], second[:, LANES : 2 * LANES], last)
        for k, piece in enumerate(pieces):
            head, tail = split(piece)
            chunks[index][k, 0, at] = head
            rests[index][k, 0, at] = tail

    for index in range(NCHUNK):
        lax.fori_loop(0, PAIRS[index], lambda at, _, index=index: one_pair(index, at), None)


def in_plane(bold, edge, side):
    cells_x, cells_y, cells_z, frames = bold.shape
    group = 256 // cells_z
    band = np.zeros((cells_z, cells_z), np.float64)
    for k in range(-REACH, REACH + 1):
        band += kernel_taps[k + REACH] * np.eye(cells_z, k=k)
    band = np.kron(np.eye(group), band).astype(np.float32)
    high = band.astype(BF)
    low = (band - high.astype(np.float32)).astype(BF)
    lanes = 3 * LANES
    pieces = [jax.ShapeDtypeStruct((5, cells_x, pairs, cells_z, LANES), BF) for pairs in PAIRS]
    piece_specs = [pl.BlockSpec((5, 1) + piece.shape[2:], lambda x: (0, x, 0, 0, 0)) for piece in pieces]
    whole = pl.BlockSpec(high.shape, lambda x: (0, 0))
    outs = pl.pallas_call(
        functools.partial(in_plane_kernel, frames=frames),
        grid=(cells_x,),
        in_specs=[
            pl.BlockSpec(memory_space=pltpu.SMEM),
            pl.BlockSpec((1, cells_y, cells_z, lanes), lambda x: (x, 0, 0, 0)),
            pl.BlockSpec((1, REACH, cells_z, lanes), lambda x: (x, 0, 0, 0)),
            whole,
            whole,
        ],
        out_specs=piece_specs * 2,
        out_shape=pieces * 2,
        scratch_shapes=[pltpu.VMEM((cells_y + 2 * REACH, cells_z, lanes), F32)],
        compiler_params=pltpu.CompilerParams(vmem_limit_bytes=VMEM),
        name="in_plane",
    )(side, bold, edge, jnp.asarray(high), jnp.asarray(low))
    return outs[:NCHUNK], outs[NCHUNK:]


def rank_kernel(row_ref, out_ref, turns_ref, *, column):
    seeds, chips = row_ref.shape[1], out_ref.shape[0]
    seed = row_ref[...]
    chip = lax.broadcasted_iota(jnp.int32, (chips, 1), 0) * column
    here = jnp.where((seed >= chip) & (seed < chip + column), 1.0, 0.0)
    earlier = lax.broadcasted_iota(jnp.int32, (seeds, seeds), 0) < lax.broadcasted_iota(jnp.int32, (seeds, seeds), 1)
    before = dot(here.astype(BF), jnp.where(earlier, 1.0, 0.0).astype(BF))
    rank = jnp.sum(here * before, axis=0, keepdims=True)
    out_ref[...] = jnp.broadcast_to(rank.astype(jnp.int32), out_ref.shape)
    turns_ref[0] = (jnp.max(rank).astype(jnp.int32) + LIST) // LIST


def part_kernel(place_ref, row_ref, rank_ref, *refs, cells, column, strip):
    chunks, rests, outs = refs[:NCHUNK], refs[NCHUNK : 2 * NCHUNK], refs[2 * NCHUNK :]
    cells_x, cells_y, cells_z = cells
    brick, side, turn = place_ref[0], place_ref[1], place_ref[2]
    half = 3 * HALF
    slots = 2 * half
    seed = row_ref[...]
    rank = rank_ref[0:1] - turn * LIST
    spot = jnp.where((rank >= 0) & (rank < LIST), (seed // column) * LIST + rank, -1)
    slot = lax.broadcasted_iota(jnp.int32, (slots, 1), 0)
    core = jnp.where(slot < half, side, 1 - side)
    slot = jnp.where(slot < half, slot, slot - half)
    which = jnp.where(slot < HALF, 0, jnp.where(slot < 2 * HALF, 1, 2))
    want = (brick - 1 + which) * LIST + core * HALF + slot - which * HALF
    want = jnp.where(want >= 0, want, -2)
    found = jnp.sum(jnp.where(spot == want, (seed + 1).astype(F32), 0.0), axis=1, keepdims=True)
    found = found.astype(jnp.int32) - 1
    seed_x = found // strip
    within = found - seed_x * strip
    seed_y = within // cells_z
    seed_z = within - seed_y * cells_z
    from_x = seed_x - brick * cells_x
    from_y = jnp.where(found < 0, -1, seed_y - side * cells_y)

    main = jnp.zeros((slots, 2 * LANES), F32)
    last = jnp.zeros((2 * slots, LANES), F32)

    def product(weights, index, pieces):
        head, tail = (
            jnp.concatenate([refs[index][k].reshape(-1, LANES) for k in pieces], axis=1) for refs in (chunks, rests)
        )
        high, low = weights
        return dot(high, head) + dot(high, tail) + dot(low, head)

    for index, pairs in enumerate(PAIRS):
        lane = lax.broadcasted_iota(jnp.int32, (1, cells_x * pairs * cells_z), 1)
        shift_z, shift_p = cells_z.bit_length() - 1, pairs.bit_length() - 1
        row = 2 * (((lane >> shift_z) & (pairs - 1)) + sum(PAIRS[:index]))
        gap = ((lane >> (shift_z + shift_p)) - from_x).astype(F32)
        taps = jnp.where(jnp.abs(gap) <= REACH, jnp.exp(gap * gap * (-1.0 / 8.0)) * (1.0 / TAP_SUM), 0.0)
        taps = jnp.where((lane & (cells_z - 1)) == seed_z, taps, 0.0)
        both = [split(jnp.where(row + odd == from_y, taps, 0.0)) for odd in range(2)]
        main = main + product(both[0], index, (0, 1)) + product(both[1], index, (2, 3))
        last = last + product([jnp.concatenate(w, axis=0) for w in zip(*both)], index, (4,))
    near = lax.broadcasted_iota(jnp.int32, (1, LANES), 1) < LANES // 2
    last = jnp.where(near, last[:slots] + pltpu.roll(last[slots:], LANES // 2, 1), 0.0)
    for k, out_ref in enumerate(outs):
        out_ref[:, : 2 * LANES] = main[k * half : (k + 1) * half]
        out_ref[:, 2 * LANES :] = last[k * half : (k + 1) * half]


def sum_kernel(own_ref, other_ref, *outs):
    for k, out_ref in enumerate(outs):
        rows = slice(k * HALF, (k + 1) * HALF)
        out_ref[...] = own_ref[rows] + other_ref[rows]


def scale_kernel(*refs, frames):
    ins, out_ref = refs[:-1], refs[-1]
    total = ins[0][...]
    for ref in ins[1:]:
        total = total + ref[...]
    var = jnp.sum(total * total, axis=1, keepdims=True) * (1.0 / frames)
    total = total * lax.rsqrt(var + 1e-06)
    half = HALF // 2
    first, second = total[:half], total[half:]
    last = first[:, 2 * LANES :] + pltpu.roll(second[:, 2 * LANES :], LANES // 2, 1)
    pieces = (first[:, :LANES], first[:, LANES : 2 * LANES], second[:, :LANES], second[:, LANES : 2 * LANES], last)
    for k, piece in enumerate(pieces):
        out_ref[k] = piece.astype(BF)


def join_kernel(*refs):
    out_ref = refs[-1]
    count = out_ref.shape[0] // (len(refs) - 1)
    for k, ref in enumerate(refs[:-1]):
        out_ref[k * count : (k + 1) * count] = ref[...].reshape((count,) + out_ref.shape[1:])


def join(pieces):
    count = pieces[0].size // math.prod(pieces[0].shape[-3:])
    shape = (count * len(pieces),) + pieces[0].shape[-3:]
    return call(join_kernel, jax.ShapeDtypeStruct(shape, pieces[0].dtype), *pieces)


def order_kernel(place_ref, row_ref, rank_ref, own_ref, other_ref, out_ref, *, column):
    side, turn = place_ref[1], place_ref[2]
    half = HALF // 2
    count = own_ref.shape[0] * half
    rank = rank_ref[0:1] - turn * LIST
    quarter = sum(jnp.where(rank >= k * half, 1, 0) for k in range(1, 4))
    part = jnp.where(side == 0, quarter, jnp.where(quarter < 2, quarter + 2, quarter - 2))
    size = own_ref.shape[0]
    fourth = size // 4
    ahead = row_ref[...] // column - place_ref[0]
    ahead = jnp.where(ahead < 0, ahead + size, ahead)
    far = ahead // fourth
    low = ahead - far * fourth
    far = jnp.where(2 * low > fourth, far + 1, far)
    block = low * 4 + jnp.where(far >= 4, far - 4, far)
    spot = part * count + block * half + rank - quarter * half
    spot = jnp.where((rank >= 0) & (rank < LIST), spot, -1)
    slot = lax.broadcasted_iota(jnp.int32, (count, 1), 0)
    picks = [jnp.where(spot - part * count == slot, 1.0, 0.0).astype(BF) for part in range(4)]

    def piece(part, k):
        ref = (own_ref, other_ref)[part // 2]
        return dot(ref[:, k].reshape(count, LANES), picks[part], (((0,), (0,)), ((), ())))

    for k in range(2):
        value = piece(0, k) + piece(1, 2 + k) + piece(2, k) + piece(3, 2 + k)
        out_ref[k * LANES : (k + 1) * LANES] = value.astype(BF)
    even, odd = piece(0, 4) + piece(2, 4), piece(1, 4) + piece(3, 4)
    last = even[: LANES // 2] + odd[LANES // 2 :]
    out_ref[2 * LANES :] = jnp.concatenate([last, jnp.zeros_like(last)], axis=0).astype(BF)


def in_order(place, row, ranks, own, other, column):
    seeds, block = row.shape[1], 128
    return pl.pallas_call(
        functools.partial(order_kernel, column=column),
        grid=(seeds // block,),
        in_specs=[
            pl.BlockSpec(memory_space=pltpu.SMEM),
            pl.BlockSpec((1, block), lambda i: (0, i)),
            pl.BlockSpec((ranks.shape[0], block), lambda i: (0, i)),
        ]
        + [pl.BlockSpec(own.shape, lambda i: (0, 0, 0, 0))] * 2,
        out_specs=pl.BlockSpec((3 * LANES, block), lambda i: (0, i)),
        out_shape=jax.ShapeDtypeStruct((3 * LANES, seeds), BF),
        compiler_params=pltpu.CompilerParams(vmem_limit_bytes=VMEM),
        name="order",
    )(place, row, ranks, own, other)


def scores_kernel(bounds_ref, own_ref, before_ref, after_ref, out_ref, *, frames, first):
    cells_x, cells_z = own_ref.shape[1], own_ref.shape[3]
    pair = first + pl.program_id(0)
    near = lax.broadcasted_iota(jnp.int32, (1, LANES), 1) < LANES // 2
    depth = lax.broadcasted_iota(jnp.int32, (cells_z, 1), 0)

    def plane(k, x):
        if x < 0:
            return before_ref[k, x + cells_x, 0].astype(F32)
        if x >= cells_x:
            return after_ref[k, x - cells_x, 0].astype(F32)
        return own_ref[k, x, 0].astype(F32)

    for x in range(cells_x):
        sums = []
        for k in range(5):
            total = kernel_taps[REACH] * plane(k, x)
            for t in range(1, REACH + 1):
                total = total + kernel_taps[REACH + t] * (plane(k, x - t) + plane(k, x + t))
            sums.append(total)
        for odd in range(2):
            last = pltpu.roll(sums[4], LANES // 2, 1) if odd else sums[4]
            pieces = (sums[2 * odd], sums[2 * odd + 1], jnp.where(near, last, 0.0))
            square = pieces[0] * pieces[0] + pieces[1] * pieces[1] + pieces[2] * pieces[2]
            var = jnp.sum(square, axis=1, keepdims=True) * (1.0 / frames)
            row = x * (bounds_ref.shape[1] // cells_x) + 2 * pair + odd
            inside = (depth >= bounds_ref[0, row]) & (depth < bounds_ref[1, row])
            scale = jnp.where(inside, lax.rsqrt(var + 1e-06), 0.0)
            for k, piece in enumerate(pieces):
                out_ref[x, odd, :, k * LANES : (k + 1) * LANES] = (piece * scale).astype(BF)


def scores(bounds, own, before, after, frames, index):
    _, cells_x, pairs, cells_z, _ = own.shape
    spec = pl.BlockSpec((5, cells_x, 1, cells_z, LANES), lambda p: (0, 0, p, 0, 0))
    return pl.pallas_call(
        functools.partial(scores_kernel, frames=frames, first=sum(PAIRS[:index])),
        grid=(pairs,),
        in_specs=[pl.BlockSpec(memory_space=pltpu.SMEM), spec, spec, spec],
        out_specs=pl.BlockSpec((cells_x, 2, cells_z, 3 * LANES), lambda p: (0, p, 0, 0)),
        out_shape=jax.ShapeDtypeStruct((cells_x, 2 * pairs, cells_z, 3 * LANES), BF),
        name="scores",
    )(bounds, own, before, after)


def correlate_kernel(table_ref, score_ref, *refs, frames):
    out_ref = refs[-1]
    corr = dot(score_ref[...].reshape(-1, table_ref.shape[0]), table_ref[...]) * (1.0 / frames)
    out_ref[...] = corr.astype(BF).reshape(out_ref.shape)


def correlate(table, score, out, shape, frames, index):
    cells_x, rows, cells_z, lanes = score.shape
    first = sum(PAIRS[:index])
    more = [] if out is None else [out]
    return pl.pallas_call(
        functools.partial(correlate_kernel, frames=frames),
        grid=(rows // 2,),
        in_specs=[
            pl.BlockSpec(table.shape, lambda p: (0, 0)),
            pl.BlockSpec((cells_x, 2, cells_z, lanes), lambda p: (0, p, 0, 0)),
        ]
        + [pl.BlockSpec(memory_space=pl.ANY)] * len(more),
        out_specs=pl.BlockSpec((cells_x, 2, cells_z, shape[-1]), lambda p: (0, first + p, 0, 0)),
        out_shape=jax.ShapeDtypeStruct(shape, BF),
        input_output_aliases={2: 0} if more else {},
        name="correlate",
    )(table, score, *more)


def call(kernel, out, *args, smem=0):
    in_specs = [pl.BlockSpec(memory_space=pltpu.SMEM)] * smem + [pl.BlockSpec(memory_space=pltpu.VMEM)] * (len(args) - smem)
    multi = isinstance(out, list)
    return pl.pallas_call(
        kernel,
        in_specs=in_specs,
        out_specs=[pl.BlockSpec(memory_space=pltpu.VMEM)] * len(out) if multi else pl.BlockSpec(memory_space=pltpu.VMEM),
        out_shape=out,
        compiler_params=pltpu.CompilerParams(vmem_limit_bytes=VMEM),
    )(*args)


def shift(value, step, flip=False, wrap=False):
    size, cores = lax.axis_size("gx"), lax.axis_size("gy")
    pairs = []
    for i in range(size):
        if wrap or 0 <= i + step < size:
            for c in range(cores):
                source = (i + step) % size * cores + (cores - 1 - c if flip else c)
                pairs.append((source, i * cores + c))
    return lax.ppermute(value, ("gx", "gy"), pairs)


def local(bold, brain_bounds, seed_index):
    frames, cells_x, cells_y, cells_z = bold.shape
    seeds = seed_index.shape[0]
    size, cores = lax.axis_size("gx"), lax.axis_size("gy")
    brick, side = lax.axis_index("gx"), lax.axis_index("gy")
    bold = jnp.transpose(bold, (1, 2, 3, 0))
    sides = side.astype(jnp.int32).reshape(1)

    send = lax.dynamic_slice_in_dim(bold, jnp.where(side == 0, cells_y - REACH, 0), REACH, axis=1)
    edge = shift(send, 0, flip=True)
    bounds = jnp.transpose(brain_bounds, (2, 0, 1)).reshape(2, cells_x * cells_y)
    edge, bounds = lax.optimization_barrier((edge, bounds))
    chunks, rests = in_plane(bold, edge, sides)
    halos = [(shift(c, -1), shift(c, 1)) for c in chunks]

    strip = cores * cells_y * cells_z
    column = cells_x * strip
    row = seed_index.reshape(1, seeds)
    ranks, turns = pl.pallas_call(
        functools.partial(rank_kernel, column=column),
        in_specs=[pl.BlockSpec(memory_space=pltpu.VMEM)],
        out_specs=[pl.BlockSpec(memory_space=pltpu.VMEM), pl.BlockSpec(memory_space=pltpu.SMEM)],
        out_shape=[jax.ShapeDtypeStruct((size, seeds), jnp.int32), jax.ShapeDtypeStruct((1,), jnp.int32)],
        name="rank",
    )(row)

    fourth = size // 4
    far_steps = [k * fourth for k in range(1, 4)]
    near_steps = [k if 2 * k <= fourth else k - fourth for k in range(1, fourth)]

    def table_of(turn):
        place = jnp.stack([brick, side, turn]).astype(jnp.int32)
        own, other = call(
            functools.partial(part_kernel, cells=(cells_x, cells_y, cells_z), column=column, strip=strip),
            [jax.ShapeDtypeStruct((3 * HALF, 3 * LANES), F32)] * 2,
            place,
            row,
            ranks,
            *chunks,
            *rests,
            smem=1,
        )
        other = shift(other, 0, flip=True)
        lists = call(sum_kernel, [jax.ShapeDtypeStruct((HALF, 3 * LANES), F32)] * 3, own, other)
        below = shift(lists[2], -1)
        above = shift(lists[0], 1)
        mine = call(
            functools.partial(scale_kernel, frames=frames),
            jax.ShapeDtypeStruct((5, HALF // 2, LANES), BF),
            lists[1],
            below,
            above,
        )
        far = [mine] + [shift(mine, step, wrap=True) for step in far_steps]
        some = join(far)
        near = [some] + [shift(some, step, wrap=True) for step in near_steps]
        every = join(near)
        other = shift(every, 0, flip=True)
        return in_order(place, row, ranks, every, other, column)

    table = table_of(jnp.int32(0))
    _, table = lax.while_loop(
        lambda s: s[0] < turns[0], lambda s: (s[0] + 1, s[1] + table_of(s[0])), (jnp.int32(1), table)
    )

    shape = (cells_x, cells_y, cells_z, seeds)
    out = None
    for index in range(NCHUNK):
        score = scores(bounds, chunks[index], *halos[index], frames, index)
        out = correlate(table, score, out, shape, frames, index)
    return out


def solution(mesh):
    placed = (P("subj", "gx", "gy", None), P("gx", "gy", "subj"), P("subj"))

    return jax.shard_map(local, mesh=mesh, in_specs=placed, out_specs=P("gx", "gy", None, "subj"), check_vma=False)
```

```python
import functools
import math

import jax
import jax.numpy as jnp
import numpy as np
from jax import lax
from jax.experimental import pallas as pl
from jax.experimental.pallas import tpu as pltpu
from jax.sharding import PartitionSpec as P


raw_taps = [math.exp(-k * k / 8.0) for k in range(-4, 5)]
kernel_taps = [t / sum(raw_taps) for t in raw_taps]
TAP_SUM = sum(raw_taps)
REACH = 4
LANES = 128
BF = jnp.bfloat16
F32 = jnp.float32
PAIRS = (4, 4, 4, 4)
NCHUNK = len(PAIRS)
HALF = 32
LIST = 2 * HALF
VMEM = 56 * 1024 * 1024


def dot(a, b, dims=(((1,), (0,)), ((), ()))):
    return lax.dot_general(a, b, dims, preferred_element_type=F32)


def split(a):
    high = a.astype(BF)
    return high, (a - high.astype(F32)).astype(BF)


def in_plane_kernel(side_ref, bold_ref, edge_ref, high_ref, low_ref, *refs, frames):
    chunks, rests, wide = refs[:NCHUNK], refs[NCHUNK : 2 * NCHUNK], refs[2 * NCHUNK]
    rows, cells_z = bold_ref.shape[1], bold_ref.shape[2]
    lanes = wide.shape[2]
    keep = lax.broadcasted_iota(jnp.int32, (1, 1, lanes), 2) < frames
    side = side_ref[0]
    taps_high, taps_low = high_ref[...], low_ref[...]
    group = taps_high.shape[0] // cells_z

    def along_z(block, count):
        block = jnp.where(keep, block, 0.0)
        mean = jnp.sum(block, axis=-1, keepdims=True) * (1.0 / frames)
        block = jnp.where(keep, block - mean, 0.0).reshape(count * cells_z, lanes)
        size = count * cells_z
        head, rest = split(block)
        th, tl = taps_high[:size, :size], taps_low[:size, :size]
        return (dot(th, head) + dot(th, rest) + dot(tl, head)).reshape(count, cells_z, lanes)

    for at in range(0, rows, group):
        wide[REACH + at : REACH + at + group] = along_z(bold_ref[0, at : at + group], group)
    edge = along_z(edge_ref[0], REACH)
    wide[:REACH] = jnp.where(side == 1, edge, 0.0)
    wide[REACH + rows :] = jnp.where(side == 1, 0.0, edge)

    def one_pair(index, at):
        first_row = 2 * (sum(PAIRS[:index]) + at)

        def along_y(row):
            total = kernel_taps[REACH] * wide[row + REACH]
            for k in range(1, REACH + 1):
                total = total + kernel_taps[REACH + k] * (wide[row + REACH - k] + wide[row + REACH + k])
            return total

        first, second = along_y(first_row), along_y(first_row + 1)
        last = first[:, 2 * LANES :] + pltpu.roll(second[:, 2 * LANES :], LANES // 2, 1)
        pieces = (first[:, :LANES], first[:, LANES : 2 * LANES], second[:, :LANES], second[:, LANES : 2 * LANES], last)
        for k, piece in enumerate(pieces):
            head, tail = split(piece)
            chunks[index][k, 0, at] = head
            rests[index][k, 0, at] = tail

    for index in range(NCHUNK):
        lax.fori_loop(0, PAIRS[index], lambda at, _, index=index: one_pair(index, at), None)


def in_plane(bold, edge, side):
    cells_x, cells_y, cells_z, frames = bold.shape
    group = 256 // cells_z
    band = np.zeros((cells_z, cells_z), np.float64)
    for k in range(-REACH, REACH + 1):
        band += kernel_taps[k + REACH] * np.eye(cells_z, k=k)
    band = np.kron(np.eye(group), band).astype(np.float32)
    high = band.astype(BF)
    low = (band - high.astype(np.float32)).astype(BF)
    lanes = 3 * LANES
    pieces = [jax.ShapeDtypeStruct((5, cells_x, pairs, cells_z, LANES), BF) for pairs in PAIRS]
    piece_specs = [pl.BlockSpec((5, 1) + piece.shape[2:], lambda x: (0, x, 0, 0, 0)) for piece in pieces]
    whole = pl.BlockSpec(high.shape, lambda x: (0, 0))
    outs = pl.pallas_call(
        functools.partial(in_plane_kernel, frames=frames),
        grid=(cells_x,),
        in_specs=[
            pl.BlockSpec(memory_space=pltpu.SMEM),
            pl.BlockSpec((1, cells_y, cells_z, lanes), lambda x: (x, 0, 0, 0)),
            pl.BlockSpec((1, REACH, cells_z, lanes), lambda x: (x, 0, 0, 0)),
            whole,
            whole,
        ],
        out_specs=piece_specs * 2,
        out_shape=pieces * 2,
        scratch_shapes=[pltpu.VMEM((cells_y + 2 * REACH, cells_z, lanes), F32)],
        compiler_params=pltpu.CompilerParams(vmem_limit_bytes=VMEM),
        name="in_plane",
    )(side, bold, edge, jnp.asarray(high), jnp.asarray(low))
    return outs[:NCHUNK], outs[NCHUNK:]


def rank_kernel(row_ref, block_ref, out_ref, turns_ref, *, column):
    seeds, chips, count = row_ref.shape[1], out_ref.shape[0], block_ref.shape[1]
    step = pl.program_id(0)
    chip = lax.broadcasted_iota(jnp.int32, (chips, 1), 0) * column

    def here(seed):
        return jnp.where((seed >= chip) & (seed < chip + column), 1.0, 0.0)

    down, across = (lax.broadcasted_iota(jnp.int32, (seeds, count), axis) for axis in (0, 1))
    earlier = jnp.where(down < across + step * count, 1.0, 0.0).astype(BF)
    before = dot(here(row_ref[...]).astype(BF), earlier)
    rank = jnp.sum(here(block_ref[...]) * before, axis=0, keepdims=True)
    out_ref[...] = jnp.broadcast_to(rank.astype(jnp.int32), out_ref.shape)
    turns = (jnp.max(rank).astype(jnp.int32) + LIST) // LIST
    turns_ref[0] = jnp.maximum(turns, jnp.where(step == 0, 0, turns_ref[0]))


def part_kernel(place_ref, row_ref, rank_ref, *refs, cells, column, strip):
    chunks, rests, outs = refs[:NCHUNK], refs[NCHUNK : 2 * NCHUNK], refs[2 * NCHUNK :]
    cells_x, cells_y, cells_z = cells
    brick, side, turn = place_ref[0], place_ref[1], place_ref[2]
    half = 3 * HALF
    slots = 2 * half
    seed = row_ref[...]
    rank = rank_ref[0:1] - turn * LIST
    spot = jnp.where((rank >= 0) & (rank < LIST), (seed // column) * LIST + rank, -1)
    slot = lax.broadcasted_iota(jnp.int32, (slots, 1), 0)
    core = jnp.where(slot < half, side, 1 - side)
    slot = jnp.where(slot < half, slot, slot - half)
    which = jnp.where(slot < HALF, 0, jnp.where(slot < 2 * HALF, 1, 2))
    want = (brick - 1 + which) * LIST + core * HALF + slot - which * HALF
    want = jnp.where(want >= 0, want, -2)
    found = jnp.sum(jnp.where(spot == want, (seed + 1).astype(F32), 0.0), axis=1, keepdims=True)
    found = found.astype(jnp.int32) - 1
    seed_x = found // strip
    within = found - seed_x * strip
    seed_y = within // cells_z
    seed_z = within - seed_y * cells_z
    from_x = seed_x - brick * cells_x
    from_y = jnp.where(found < 0, -1, seed_y - side * cells_y)

    main = jnp.zeros((slots, 2 * LANES), F32)
    last = jnp.zeros((2 * slots, LANES), F32)

    def product(weights, index, pieces):
        head, tail = (
            jnp.concatenate([refs[index][k].reshape(-1, LANES) for k in pieces], axis=1) for refs in (chunks, rests)
        )
        high, low = weights
        return dot(high, head) + dot(high, tail) + dot(low, head)

    for index, pairs in enumerate(PAIRS):
        lane = lax.broadcasted_iota(jnp.int32, (1, cells_x * pairs * cells_z), 1)
        shift_z, shift_p = cells_z.bit_length() - 1, pairs.bit_length() - 1
        row = 2 * (((lane >> shift_z) & (pairs - 1)) + sum(PAIRS[:index]))
        gap = ((lane >> (shift_z + shift_p)) - from_x).astype(F32)
        taps = jnp.where(jnp.abs(gap) <= REACH, jnp.exp(gap * gap * (-1.0 / 8.0)) * (1.0 / TAP_SUM), 0.0)
        taps = jnp.where((lane & (cells_z - 1)) == seed_z, taps, 0.0)
        both = [split(jnp.where(row + odd == from_y, taps, 0.0)) for odd in range(2)]
        main = main + product(both[0], index, (0, 1)) + product(both[1], index, (2, 3))
        last = last + product([jnp.concatenate(w, axis=0) for w in zip(*both)], index, (4,))
    near = lax.broadcasted_iota(jnp.int32, (1, LANES), 1) < LANES // 2
    last = jnp.where(near, last[:slots] + pltpu.roll(last[slots:], LANES // 2, 1), 0.0)
    for k, out_ref in enumerate(outs):
        out_ref[:, : 2 * LANES] = main[k * half : (k + 1) * half]
        out_ref[:, 2 * LANES :] = last[k * half : (k + 1) * half]


def sum_kernel(own_ref, other_ref, *outs):
    for k, out_ref in enumerate(outs):
        rows = slice(k * HALF, (k + 1) * HALF)
        out_ref[...] = own_ref[rows] + other_ref[rows]


def scale_kernel(*refs, frames):
    ins, out_ref = refs[:-1], refs[-1]
    total = ins[0][...]
    for ref in ins[1:]:
        total = total + ref[...]
    var = jnp.sum(total * total, axis=1, keepdims=True) * (1.0 / frames)
    total = total * lax.rsqrt(var + 1e-06)
    half = HALF // 2
    first, second = total[:half], total[half:]
    last = first[:, 2 * LANES :] + pltpu.roll(second[:, 2 * LANES :], LANES // 2, 1)
    pieces = (first[:, :LANES], first[:, LANES : 2 * LANES], second[:, :LANES], second[:, LANES : 2 * LANES], last)
    for k, piece in enumerate(pieces):
        out_ref[k] = piece.astype(BF)


def join_kernel(*refs):
    out_ref = refs[-1]
    count = out_ref.shape[0] // (len(refs) - 1)
    for k, ref in enumerate(refs[:-1]):
        out_ref[k * count : (k + 1) * count] = ref[...].reshape((count,) + out_ref.shape[1:])


def join(pieces):
    count = pieces[0].size // math.prod(pieces[0].shape[-3:])
    shape = (count * len(pieces),) + pieces[0].shape[-3:]
    return call(join_kernel, jax.ShapeDtypeStruct(shape, pieces[0].dtype), *pieces)


def order_kernel(place_ref, row_ref, rank_ref, own_ref, other_ref, out_ref, *, column, both_ways):
    side, turn = place_ref[1], place_ref[2]
    half = HALF // 2
    count = own_ref.shape[0] * half
    rank = rank_ref[0:1] - turn * LIST
    quarter = sum(jnp.where(rank >= k * half, 1, 0) for k in range(1, 4))
    part = jnp.where(side == 0, quarter, jnp.where(quarter < 2, quarter + 2, quarter - 2))
    size = own_ref.shape[0]
    fourth = size // 4
    ahead = row_ref[...] // column - place_ref[0]
    ahead = jnp.where(ahead < 0, ahead + size, ahead)
    far = ahead // fourth
    low = ahead - far * fourth
    if both_ways:
        far = jnp.where(2 * low > fourth, far + 1, far)
    block = low * 4 + jnp.where(far >= 4, far - 4, far)
    spot = part * count + block * half + rank - quarter * half
    spot = jnp.where((rank >= 0) & (rank < LIST), spot, -1)
    slot = lax.broadcasted_iota(jnp.int32, (count, 1), 0)
    picks = [jnp.where(spot - part * count == slot, 1.0, 0.0).astype(BF) for part in range(4)]

    def piece(part, k):
        ref = (own_ref, other_ref)[part // 2]
        return dot(ref[:, k].reshape(count, LANES), picks[part], (((0,), (0,)), ((), ())))

    for k in range(2):
        value = piece(0, k) + piece(1, 2 + k) + piece(2, k) + piece(3, 2 + k)
        out_ref[k * LANES : (k + 1) * LANES] = value.astype(BF)
    even, odd = piece(0, 4) + piece(2, 4), piece(1, 4) + piece(3, 4)
    last = even[: LANES // 2] + odd[LANES // 2 :]
    out_ref[2 * LANES :] = jnp.concatenate([last, jnp.zeros_like(last)], axis=0).astype(BF)


def in_order(place, row, ranks, own, other, column, both_ways):
    seeds, block = row.shape[1], 256
    return pl.pallas_call(
        functools.partial(order_kernel, column=column, both_ways=both_ways),
        grid=(seeds // block,),
        in_specs=[
            pl.BlockSpec(memory_space=pltpu.SMEM),
            pl.BlockSpec((1, block), lambda i: (0, i)),
            pl.BlockSpec((ranks.shape[0], block), lambda i: (0, i)),
        ]
        + [pl.BlockSpec(own.shape, lambda i: (0, 0, 0, 0))] * 2,
        out_specs=pl.BlockSpec((3 * LANES, block), lambda i: (0, i)),
        out_shape=jax.ShapeDtypeStruct((3 * LANES, seeds), BF),
        compiler_params=pltpu.CompilerParams(vmem_limit_bytes=VMEM),
        name="order",
    )(place, row, ranks, own, other)


def scores_kernel(bounds_ref, own_ref, before_ref, after_ref, *refs, frames, first):
    out_ref = refs[-1]
    cells_x, cells_z = own_ref.shape[1], own_ref.shape[3]
    pair = first + pl.program_id(0)
    near = lax.broadcasted_iota(jnp.int32, (1, LANES), 1) < LANES // 2
    depth = lax.broadcasted_iota(jnp.int32, (cells_z, 1), 0)

    def plane(k, x):
        if x < 0:
            return before_ref[k, x + cells_x, 0].astype(F32)
        if x >= cells_x:
            return after_ref[k, x - cells_x, 0].astype(F32)
        return own_ref[k, x, 0].astype(F32)

    for x in range(cells_x):
        sums = []
        for k in range(5):
            total = kernel_taps[REACH] * plane(k, x)
            for t in range(1, REACH + 1):
                total = total + kernel_taps[REACH + t] * (plane(k, x - t) + plane(k, x + t))
            sums.append(total)
        for odd in range(2):
            last = pltpu.roll(sums[4], LANES // 2, 1) if odd else sums[4]
            pieces = (sums[2 * odd], sums[2 * odd + 1], jnp.where(near, last, 0.0))
            square = pieces[0] * pieces[0] + pieces[1] * pieces[1] + pieces[2] * pieces[2]
            var = jnp.sum(square, axis=1, keepdims=True) * (1.0 / frames)
            row = x * (bounds_ref.shape[1] // cells_x) + 2 * pair + odd
            inside = (depth >= bounds_ref[0, row]) & (depth < bounds_ref[1, row])
            scale = jnp.where(inside, lax.rsqrt(var + 1e-06), 0.0)
            for k, piece in enumerate(pieces):
                out_ref[x, odd, :, k * LANES : (k + 1) * LANES] = (piece * scale).astype(BF)


def scores(bounds, own, before, after, out, frames, index):
    _, cells_x, pairs, cells_z, _ = own.shape
    first = sum(PAIRS[:index])
    spec = pl.BlockSpec((5, cells_x, 1, cells_z, LANES), lambda p: (0, 0, p, 0, 0))
    more = [] if out is None else [out]
    return pl.pallas_call(
        functools.partial(scores_kernel, frames=frames, first=first),
        grid=(pairs,),
        in_specs=[pl.BlockSpec(memory_space=pltpu.SMEM), spec, spec, spec]
        + [pl.BlockSpec(memory_space=pl.ANY)] * len(more),
        out_specs=pl.BlockSpec((cells_x, 2, cells_z, 3 * LANES), lambda p: (0, first + p, 0, 0)),
        out_shape=jax.ShapeDtypeStruct((cells_x, 2 * sum(PAIRS), cells_z, 3 * LANES), BF),
        input_output_aliases={4: 0} if more else {},
        name="scores",
    )(bounds, own, before, after, *more)


def correlate_kernel(table_ref, score_ref, out_ref, *, frames):
    corr = dot(score_ref[...].reshape(-1, table_ref.shape[0]), table_ref[...]) * (1.0 / frames)
    out_ref[...] = corr.astype(BF).reshape(out_ref.shape)


def correlate(table, score, frames):
    cells_x, rows, cells_z, lanes = score.shape
    block, seeds = 4, table.shape[1]
    return pl.pallas_call(
        functools.partial(correlate_kernel, frames=frames),
        grid=(rows // block,),
        in_specs=[
            pl.BlockSpec(table.shape, lambda p: (0, 0)),
            pl.BlockSpec((cells_x, block, cells_z, lanes), lambda p: (0, p, 0, 0)),
        ],
        out_specs=pl.BlockSpec((cells_x, block, cells_z, seeds), lambda p: (0, p, 0, 0)),
        out_shape=jax.ShapeDtypeStruct((cells_x, rows, cells_z, seeds), BF),
        compiler_params=pltpu.CompilerParams(vmem_limit_bytes=VMEM),
        name="correlate",
    )(table, score)


def call(kernel, out, *args, smem=0):
    in_specs = [pl.BlockSpec(memory_space=pltpu.SMEM)] * smem + [pl.BlockSpec(memory_space=pltpu.VMEM)] * (len(args) - smem)
    multi = isinstance(out, list)
    return pl.pallas_call(
        kernel,
        in_specs=in_specs,
        out_specs=[pl.BlockSpec(memory_space=pltpu.VMEM)] * len(out) if multi else pl.BlockSpec(memory_space=pltpu.VMEM),
        out_shape=out,
        compiler_params=pltpu.CompilerParams(vmem_limit_bytes=VMEM),
    )(*args)


def shift(value, step, flip=False, wrap=False):
    size, cores = lax.axis_size("gx"), lax.axis_size("gy")
    pairs = []
    for i in range(size):
        if wrap or 0 <= i + step < size:
            for c in range(cores):
                source = (i + step) % size * cores + (cores - 1 - c if flip else c)
                pairs.append((source, i * cores + c))
    return lax.ppermute(value, ("gx", "gy"), pairs)


def local(bold, brain_bounds, seed_index):
    frames, cells_x, cells_y, cells_z = bold.shape
    seeds = seed_index.shape[0]
    size, cores = lax.axis_size("gx"), lax.axis_size("gy")
    brick, side = lax.axis_index("gx"), lax.axis_index("gy")
    bold = jnp.transpose(bold, (1, 2, 3, 0))
    sides = side.astype(jnp.int32).reshape(1)

    send = lax.dynamic_slice_in_dim(bold, jnp.where(side == 0, cells_y - REACH, 0), REACH, axis=1)
    edge = shift(send, 0, flip=True)
    bounds = jnp.transpose(brain_bounds, (2, 0, 1)).reshape(2, cells_x * cells_y)
    edge, bounds = lax.optimization_barrier((edge, bounds))
    chunks, rests = in_plane(bold, edge, sides)
    halos = [(shift(c, -1), shift(c, 1)) for c in chunks]

    strip = cores * cells_y * cells_z
    column = cells_x * strip
    row = seed_index.reshape(1, seeds)
    ranks, turns = pl.pallas_call(
        functools.partial(rank_kernel, column=column),
        grid=(seeds // 256,),
        in_specs=[pl.BlockSpec((1, seeds), lambda i: (0, 0)), pl.BlockSpec((1, 256), lambda i: (0, i))],
        out_specs=[pl.BlockSpec((size, 256), lambda i: (0, i)), pl.BlockSpec(memory_space=pltpu.SMEM)],
        out_shape=[jax.ShapeDtypeStruct((size, seeds), jnp.int32), jax.ShapeDtypeStruct((1,), jnp.int32)],
        name="rank",
    )(row, row)

    fourth = size // 4
    far_steps = [k * fourth for k in range(1, 4)]
    near_steps = [k if 2 * k <= fourth else k - fourth for k in range(1, fourth)]

    def table_of(turn, doubling):
        place = jnp.stack([brick, side, turn]).astype(jnp.int32)
        own, other = call(
            functools.partial(part_kernel, cells=(cells_x, cells_y, cells_z), column=column, strip=strip),
            [jax.ShapeDtypeStruct((3 * HALF, 3 * LANES), F32)] * 2,
            place,
            row,
            ranks,
            *chunks,
            *rests,
            smem=1,
        )
        other = shift(other, 0, flip=True)
        lists = call(sum_kernel, [jax.ShapeDtypeStruct((HALF, 3 * LANES), F32)] * 3, own, other)
        below = shift(lists[2], -1)
        above = shift(lists[0], 1)
        mine = call(
            functools.partial(scale_kernel, frames=frames),
            jax.ShapeDtypeStruct((5, HALF // 2, LANES), BF),
            lists[1],
            below,
            above,
        )
        far = [mine] + [shift(mine, step, wrap=True) for step in far_steps]
        some = join(far)
        if doubling:
            every, step = some, 1
            while step < fourth:
                every = join([every, shift(every, step, wrap=True)])
                step *= 2
        else:
            near = [some] + [shift(some, step, wrap=True) for step in near_steps]
            every = join(near)
        other = shift(every, 0, flip=True)
        return in_order(place, row, ranks, every, other, column, not doubling)

    table = table_of(jnp.int32(0), False)
    _, table = lax.while_loop(
        lambda s: s[0] < turns[0], lambda s: (s[0] + 1, s[1] + table_of(s[0], True)), (jnp.int32(1), table)
    )

    score = None
    for index in range(NCHUNK):
        score = scores(bounds, chunks[index], *halos[index], score, frames, index)
    return correlate(table, score, frames)


def solution(mesh):
    placed = (P("subj", "gx", "gy", None), P("gx", "gy", "subj"), P("subj"))

    return jax.shard_map(local, mesh=mesh, in_specs=placed, out_specs=P("gx", "gy", None, "subj"), check_vma=False)
```
